32 devices in a mesh: grp: 4 (over y, core), hlp: 8 (over z, x).
Axes of the slice: x: 2, y: 2, z: 4, core: 2. Of those that a mesh axis runs over, the one named last changes fastest.
Arguments:
- pivot_inverse: bfloat16 [4, 2048, 2048], P('grp', 'hlp'), may hold values from -1 to 2, as said below
- cross_block: bfloat16 [4, 3584, 2048], P('grp', 'hlp'), may hold values from -0.375 to 0.375
- contrib_block: float32 [4, 3584, 3584], P('grp', 'hlp'), may hold values from -3 to 3, as said below
- pivot_sources: bfloat16 [4, 2048, 512], P('grp', 'hlp'), may hold values from -6 to 6
- contrib_sources: bfloat16 [4, 3584, 512], P('grp', 'hlp'), may hold values from -6 to 6
- ext_map: int32 [4, 3584], P('grp', 'hlp'), may hold values from 0 to 7167, as said below
- parent_front: float32 [7168, 7168], P(('grp', 'hlp')), may hold values from -6 to 6, as said below
- parent_rhs: float32 [7168, 512], P(('grp', 'hlp')), may hold values from -6 to 6
Outputs:
- solved: bfloat16 [4, 2048, 512], P('grp', 'hlp')
- front_out: float32 [7168, 7168], P(('grp', 'hlp'))
- rhs_out: float32 [7168, 512], P(('grp', 'hlp'))
The draws below stay inside these ranges and needn't reach their ends.
Inputs may be any that keep to these rules, and one draw needn't show every extreme that they name: `ext_map`: the 3584 entries of one child are distinct. Within each aligned block of 448 entries of a child, at most 28 entries fall into any one aligned block of 224 parent rows, and exactly 28 fall into some such block. `pivot_inverse`: lower triangular with positive diagonal. `contrib_block`: each child's block is symmetric. `parent_front`: Symmetric.
All inputs are finite; a program needn't handle non-finite values.
Results may differ from the reference program's by a relative error of at most 0.0043.
Values may be sent and summed in bfloat16 or wider, within the bound.
No kernel may reach another device: no remote copies, remote signals or barrier semaphores. Data moves between devices by JAX's collectives and lax.ppermute only.
A program may use at most 128 MiB of HBM per device.

```python
import jax
import jax.numpy as jnp
from jax import lax

P_SIZE = 2048
C = 3584
NP = 7168
NSRC = 512
GROUPS = 4
CAP = 28
N_HLP = 8
DEVICES = 32


def draw_pivot_inverse(key, part):
    first_key, second_key = jax.random.split(key)
    rows_at = jnp.arange(P_SIZE)[:, None]
    cols_at = jnp.arange(P_SIZE)[None, :]
    below = (cols_at < rows_at).astype(jnp.float32)
    diagonal = jnp.exp(jax.random.uniform(first_key, (GROUPS, P_SIZE), jnp.float32, jnp.log(0.5), jnp.log(2.0)))
    strict_part = jnp.clip(jax.random.normal(second_key, (GROUPS, P_SIZE, P_SIZE), jnp.float32), -4.0, 4.0) * (0.6 / jnp.sqrt(1.0 * P_SIZE))
    eye_part = (cols_at == rows_at).astype(jnp.float32)
    whole = strict_part * below[None] + eye_part[None] * diagonal[:, :, None]
    return whole.astype(jnp.bfloat16)


def symmetric_noise(key, shape, scale, bound):
    raw = jax.random.normal(key, shape, jnp.float32)
    mirrored = (raw + jnp.swapaxes(raw, -1, -2)) * 0.70710678
    return jnp.clip(mirrored * scale, -bound, bound)


def draw_contrib_block(key, part):
    return symmetric_noise(jax.random.fold_in(key, 11), (GROUPS, C, C), 0.5, 3.0)


def draw_parent_front(key, part):
    return symmetric_noise(jax.random.fold_in(key, 23), (NP, NP), 1.0, 6.0)


def draw_ext_map(key, part):
    owned = NP // DEVICES
    per_source = C // N_HLP
    slot_at = jnp.arange(NP)
    owner_of = slot_at // owned
    within = slot_at % owned
    helper_of = slot_at % N_HLP
    usable_rank = within // N_HLP

    def one_group(group_key):
        perm_key, source_keys = jax.random.split(group_key)
        slot_perm = jax.vmap(lambda one_key: jax.random.permutation(one_key, owned))(jax.random.split(perm_key, DEVICES))
        rows_flat = (jnp.arange(DEVICES)[:, None] * owned + slot_perm).reshape(-1)

        def one_source(helper, source_key):
            first_key, second_key = jax.random.split(source_key)
            usable = (helper_of == helper) & (usable_rank < CAP)
            pick_order = jax.random.permutation(second_key, NP)
            chosen_slot = jnp.argmin(jnp.where(usable, pick_order, pick_order + 2 * NP))
            chosen = chosen_slot // owned
            priority = jax.random.permutation(first_key, NP)
            priority = jnp.where(owner_of == chosen, priority - NP, priority)
            priority = jnp.where(usable, priority, priority + 3 * NP)
            ranking = jnp.argsort(priority)
            return rows_flat[ranking[:per_source]]
        picked = jax.vmap(one_source)(jnp.arange(N_HLP), jax.random.split(source_keys, N_HLP))
        return picked.reshape(C)
    return jax.vmap(one_group)(jax.random.split(key, GROUPS)).astype(jnp.int32)


def level_of(own_key, shape, cuts, low, largest):
    def one(axis_at, parts):
        steps = jax.random.uniform(jax.random.fold_in(jax.random.fold_in(own_key, 6), axis_at), (parts,), jnp.float32, low / len(cuts), largest / len(cuts))
        return jnp.repeat(jnp.exp(steps), shape[axis_at] // parts).reshape((-1,) + (1,) * (len(shape) - axis_at - 1))

    loudness = one(*cuts[0])
    for cut in cuts[1:]:
        loudness = loudness * one(*cut)
    return loudness


def gaussian(own_key, extent, deviation, limit, shards=(), kind=jnp.bfloat16):
    factor_of = level_of(own_key, extent, shards, -0.22, 0.18) if shards else 1.0
    values = jax.random.normal(own_key, extent, jnp.float32) * deviation * factor_of
    return jnp.minimum(jnp.maximum(values, -limit), limit).astype(kind)


def setup_inputs(seed: int = 0) -> dict:
    seeds = jax.random.split(jax.random.key(seed), 9)
    return {
        "pivot_inverse": draw_pivot_inverse(jax.random.fold_in(seeds[8], 71), 0),
        "cross_block": gaussian(seeds[1], (GROUPS, C, P_SIZE), (P_SIZE // 8) ** -0.5, 0.375, ((0, 4), (1, 8))),
        "contrib_block": draw_contrib_block(jax.random.fold_in(seeds[8], 71), 0),
        "pivot_sources": gaussian(seeds[3], (GROUPS, P_SIZE, NSRC), 1.0, 6.0, ((0, 4), (1, 8))),
        "contrib_sources": gaussian(seeds[4], (GROUPS, C, NSRC), 1.0, 6.0, ((0, 4), (1, 8))),
        "ext_map": draw_ext_map(jax.random.fold_in(seeds[8], 71), 0),
        "parent_front": draw_parent_front(jax.random.fold_in(seeds[8], 71), 0),
        "parent_rhs": gaussian(seeds[7], (NP, NSRC), 1.0, 6.0, ((0, 32),), jnp.float32),
    }


def reference(pivot_inverse, cross_block, contrib_block, pivot_sources, contrib_sources, ext_map, parent_front, parent_rhs):
    def one_front(running, members):
        parent, right_side = running
        inverse, coupling, contrib, piv_source, con_source, targets = members
        lower_part = jnp.dot(coupling, inverse.T, preferred_element_type=jnp.float32).astype(jnp.bfloat16)
        schur_rows = contrib - jnp.dot(lower_part, lower_part.T, preferred_element_type=jnp.float32)
        solved = jnp.dot(inverse, piv_source, preferred_element_type=jnp.float32).astype(jnp.bfloat16)
        update = con_source.astype(jnp.float32) - jnp.dot(lower_part, solved, preferred_element_type=jnp.float32)
        parent = parent.at[targets[:, None], targets[None, :]].add(schur_rows)
        right_side = right_side.at[targets].add(update)
        return (parent, right_side), solved

    (front_out, rhs_out), solved = lax.scan(
        one_front, (parent_front, parent_rhs),
        (pivot_inverse, cross_block, contrib_block, pivot_sources, contrib_sources, ext_map))
    return solved, front_out, rhs_out
```

```python
import functools

import jax
import jax.numpy as jnp
import numpy as np
from jax import lax
from jax.experimental import pallas as pl
from jax.experimental.pallas import tpu as pltpu
from jax.sharding import PartitionSpec as P

BOTH = ("grp", "hlp")
F32 = jnp.float32
BF16 = jnp.bfloat16


def round_up(value, multiple):
    return -(-value // multiple) * multiple


class Plan:
    def __init__(self, groups, helpers):
        self.groups, self.helpers = groups, helpers
        self.half = helpers // 2
        self.ring = list(range(0, helpers, 2)) + list(range(helpers - 1, 0, -2))
        self.place = {h: i for i, h in enumerate(self.ring)}

    def at(self, helper, shift):
        return self.ring[(self.place[helper] + shift) % self.helpers]

    def sign(self, group):
        return 1 if group % 2 == 0 else -1

    def shift_perm(self, direction):
        return [
            (g * self.helpers + h, g * self.helpers + self.at(h, direction))
            for g in range(self.groups)
            for h in range(self.helpers)
        ]

    def side_perm(self):
        return [
            (g * self.helpers + h, g * self.helpers + self.at(h, self.sign(g)))
            for g in range(self.groups)
            for h in range(self.helpers)
        ]

    def partners(self):
        return np.array(
            [
                [[self.at(h, -self.sign(g) * d) for d in range(self.half + 1)] for h in range(self.helpers)]
                for g in range(2)
            ],
            np.int32,
        )

    def pieces(self):
        source = np.zeros((self.groups, self.helpers, self.helpers), np.int32)
        rows = np.zeros_like(source)
        for g in range(self.groups):
            for c in range(self.helpers):
                for e in range(self.helpers):
                    if e <= self.half:
                        source[g, c, e] = rows[g, c, e] = self.at(c, self.sign(g) * e)
                    else:
                        source[g, c, e] = c
                        rows[g, c, e] = self.at(c, -self.sign(g) * (e - self.half))
        return source, rows


def nt(a, b):
    return lax.dot_general(a, b, (((1,), (1,)), ((), ())), preferred_element_type=F32)


def nn(a, b):
    return jnp.dot(a, b, preferred_element_type=F32)


def assemble_kernel(
    source_ref, recv_ref, rowidx_ref, rhsidx_ref, slotcol_ref, tilecol_ref, parent_ref, prhs_ref,
    out_ref, rhs_ref, wide, mixed, slots, outt,
    *, helpers, devices, rows_per, block, owned, pitch, rhs_half,
):
    g = pl.program_id(0)
    half = helpers // 2
    lanes = half * block

    @pl.when(g == 0)
    def _():
        outt[...] = jnp.zeros_like(outt)
        rhs_ref[...] = prhs_ref[...]

    wide[...] = recv_ref[...].astype(F32)

    row_iota = lax.broadcasted_iota(jnp.int32, (owned, helpers * rows_per), 0)
    for f in range(2):
        pick = (rhsidx_ref[f] == row_iota).astype(BF16)
        at = slice(f * rhs_half, (f + 1) * rhs_half)
        rhs_ref[:, at] += nn(pick, recv_ref[:, lanes:])

    slot_iota = lax.broadcasted_iota(jnp.int32, (devices * pitch, block), 0)

    def place(c, carry):
        for e in range(helpers):
            h = source_ref[(g * helpers + c) * helpers + e]
            first = pl.multiple_of(h * rows_per, 8)
            p = e % half if e != half else 0
            mixed[e * rows_per : (e + 1) * rows_per, :] = wide[
                pl.ds(first, rows_per), p * block : (p + 1) * block
            ]
        pick = (rowidx_ref[0, c] == row_iota).astype(BF16)
        rows = nn(pick, mixed[...].astype(BF16)).astype(BF16)
        spread = (slotcol_ref[0, c] == slot_iota).astype(BF16)
        slots[c] = nt(spread, rows).astype(BF16)
        return carry

    lax.fori_loop(0, helpers, place, 0)

    col_iota = lax.broadcasted_iota(jnp.int32, (owned, helpers * pitch), 0)

    def tile(t, carry):
        at = pl.ds(pl.multiple_of(t * pitch, pitch), pitch)
        stacked = jnp.concatenate([slots[c, at, :] for c in range(helpers)], axis=0)
        pick = (tilecol_ref[0, t] == col_iota).astype(BF16)
        to = pl.ds(pl.multiple_of(t * owned, 8), owned)
        outt[to, :] += nn(pick, stacked)
        return carry

    lax.fori_loop(0, devices, tile, 0)

    @pl.when(g == pl.num_programs(0) - 1)
    def _():
        step = 128
        for b in range(devices * owned // step):
            at = slice(b * step, (b + 1) * step)
            out_ref[:, at] = parent_ref[:, at] + outt[at, :].T


def on_device(
    pivot_inverse, cross_block, contrib_block, pivot_sources, contrib_sources, ext_map, parent_front, parent_rhs
):
    helpers = lax.axis_size("hlp")
    groups = lax.axis_size("grp")
    devices = helpers * groups
    plan = Plan(groups, helpers)
    half = plan.half
    group, helper = lax.axis_index("grp"), lax.axis_index("hlp")
    me = group * helpers + helper
    inverse, coupling, contrib = pivot_inverse[0], cross_block[0], contrib_block[0]
    pivots = inverse.shape[0]
    block, width = contrib.shape
    nsrc = pivot_sources.shape[2]
    owned, parent_width = parent_front.shape
    cap = max(1, 2 * width // (helpers * devices))
    rows_per = round_up(2 * cap, 8)
    pitch = round_up(cap, 16)
    rhs_half = nsrc // 2
    order = jnp.asarray(plan.partners())[group % 2, helper]

    maps = lax.all_to_all(jnp.broadcast_to(ext_map, (devices, block)), BOTH, 0, 0, tiled=True)

    own = jnp.concatenate([inverse, pivot_sources[0]], axis=1)
    ahead, behind = plan.shift_perm(1), plan.shift_perm(-1)
    ring = jnp.asarray(np.array(plan.ring, np.int32))
    place = jnp.asarray(np.array([plan.place[h] for h in range(helpers)], np.int32))[helper]
    arrived = [(own, helper)]
    forth = back = own
    for s in range(1, half):
        forth = lax.ppermute(forth, BOTH, ahead)
        back = lax.ppermute(back, BOTH, behind)
        arrived.append((forth, ring[(place - s) % helpers]))
        arrived.append((back, ring[(place + s) % helpers]))
    cut = pivots // 2
    last = jnp.concatenate(
        [lax.ppermute(forth[:cut], BOTH, ahead), lax.ppermute(back[cut:], BOTH, behind)], axis=0
    )
    arrived.append((last, ring[(place + half) % helpers]))
    full = inverse.shape[1]
    lower = jnp.zeros((block, full), BF16)
    gathered = jnp.zeros((full, full + nsrc), BF16)
    for piece, owner_of in arrived:
        part = nt(coupling, piece[:, :full]).astype(BF16)
        lower = lax.dynamic_update_slice(lower, part, (0, owner_of * pivots))
        gathered = lax.dynamic_update_slice(gathered, piece, (owner_of * pivots, 0))

    side = plan.side_perm()
    factors = [lower]
    for d in range(half):
        factors.append(lax.ppermute(factors[-1], BOTH, side))

    solved_all = nn(gathered[:, :full], gathered[:, full:]).astype(BF16)
    solved = lax.dynamic_slice(solved_all, (helper * pivots, 0), (pivots, nsrc))
    update = (contrib_sources[0].astype(F32) - nn(lower, solved_all)).astype(BF16)

    owners = maps // owned
    local = maps - owners * owned
    same = owners[:, :, None] == owners[:, None, :]
    earlier = jnp.asarray(np.tril(np.ones((block, block), bool), -1))
    rank = jnp.sum((same & earlier[None]).astype(jnp.int32), axis=2)
    code = owners * rows_per + rank

    row_at = lax.broadcasted_iota(jnp.int32, (devices * rows_per, block), 0)

    def picker(helper_of, f):
        mine = lax.dynamic_index_in_dim(code, group * helpers + helper_of, 0, keepdims=True)
        return (mine + f * cap == row_at).astype(BF16)

    first = picker(helper, 0)
    second = [picker(order[d], 1) for d in range(half)]
    schur = []
    for d in range(half + 1):
        cols = lax.dynamic_slice(contrib, (0, order[d] * block), (block, block))
        schur.append((cols - nt(lower, factors[d])).astype(BF16))
    chunks = []
    for p in range(half):
        other = schur[half] if p == 0 else schur[p].T
        chunks.append(
            nn(
                jnp.concatenate([first, second[p]], axis=1), jnp.concatenate([schur[p], other], axis=0)
            ).astype(BF16)
        )
    chunks.append(
        nn(
            jnp.concatenate([first, second[0]], axis=1),
            jnp.concatenate([update[:, :rhs_half], update[:, rhs_half:]], axis=0),
        ).astype(BF16)
    )
    send = jnp.concatenate(chunks, axis=1)
    message = send.shape[1]
    recv = lax.all_to_all(send.reshape(devices, rows_per, message), BOTH, 0, 0, tiled=True)
    recv = recv.reshape(devices * rows_per, message)

    mine = owners == me
    ranks = jnp.arange(cap)[None, :, None]
    hit = mine[:, None, :] & (rank[:, None, :] == ranks)
    slot_row = jnp.sum(jnp.where(hit, local[:, None, :] + 1, 0), axis=2) - 1
    slot_row = slot_row.reshape(groups, helpers, cap)
    source, row_block = plan.pieces()
    nothing = -jnp.ones((groups, helpers, helpers, rows_per), jnp.int32)
    rowidx = nothing
    for e in range(helpers):
        f = 0 if e < half else 1
        rows_of = jnp.take_along_axis(slot_row, jnp.asarray(row_block[:, :, e])[:, :, None], axis=1)
        rowidx = rowidx.at[:, :, e, f * cap : (f + 1) * cap].set(rows_of)
    rowidx = rowidx.reshape(groups, helpers, 1, helpers * rows_per)
    rhsidx = jnp.stack(
        [nothing[:, 0].at[:, :, f * cap : (f + 1) * cap].set(slot_row) for f in range(2)], axis=1
    ).reshape(groups * 2, 1, helpers * rows_per)
    slot = owners * pitch + rank
    slotcol = slot.reshape(groups, helpers, 1, block)
    every = jnp.arange(devices * pitch)[None, :, None]
    tilecol = jnp.sum(jnp.where(slot[:, None, :] == every, local[:, None, :] + 1, 0), axis=2) - 1
    tilecol = tilecol.reshape(groups, helpers, devices, pitch).transpose(0, 2, 1, 3)
    tilecol = tilecol.reshape(groups, devices, 1, helpers * pitch)

    rows_in = helpers * rows_per
    kernel = functools.partial(
        assemble_kernel,
        helpers=helpers, devices=devices, rows_per=rows_per, block=block, owned=owned, pitch=pitch,
        rhs_half=rhs_half,
    )
    front_out, rhs_out = pl.pallas_call(
        kernel,
        grid_spec=pltpu.PrefetchScalarGridSpec(
            num_scalar_prefetch=1,
            grid=(groups,),
            in_specs=[
                pl.BlockSpec((rows_in, message), lambda g, s: (g, 0)),
                pl.BlockSpec((1, helpers, 1, rows_in), lambda g, s: (g, 0, 0, 0)),
                pl.BlockSpec((2, 1, rows_in), lambda g, s: (g, 0, 0)),
                pl.BlockSpec((1, helpers, 1, block), lambda g, s: (g, 0, 0, 0)),
                pl.BlockSpec((1, devices, 1, helpers * pitch), lambda g, s: (g, 0, 0, 0)),
                pl.BlockSpec((owned, parent_width), lambda g, s: (0, 0)),
                pl.BlockSpec((owned, nsrc), lambda g, s: (0, 0)),
            ],
            out_specs=[
                pl.BlockSpec((owned, parent_width), lambda g, s: (0, 0)),
                pl.BlockSpec((owned, nsrc), lambda g, s: (0, 0)),
            ],
            scratch_shapes=[
                pltpu.VMEM((rows_in, message), F32),
                pltpu.VMEM((rows_in, block), F32),
                pltpu.VMEM((helpers, devices * pitch, owned), BF16),
                pltpu.VMEM((parent_width, owned), F32),
            ],
        ),
        out_shape=[
            jax.ShapeDtypeStruct((owned, parent_width), F32),
            jax.ShapeDtypeStruct((owned, nsrc), F32),
        ],
        compiler_params=pltpu.CompilerParams(vmem_limit_bytes=60 * 1024 * 1024),
        name="assemble",
    )(
        jnp.asarray(source.reshape(-1)), recv, rowidx, rhsidx, slotcol, tilecol, parent_front, parent_rhs
    )
    return solved[None], front_out, rhs_out


def solution(mesh):
    return jax.shard_map(
        on_device,
        mesh=mesh,
        in_specs=(
            P("grp", "hlp", None),
            P("grp", "hlp", None),
            P("grp", "hlp", None),
            P("grp", "hlp", None),
            P("grp", "hlp", None),
            P("grp", "hlp"),
            P(("grp", "hlp"), None),
            P(("grp", "hlp"), None),
        ),
        out_specs=(P("grp", "hlp", None), P(("grp", "hlp"), None), P(("grp", "hlp"), None)),
        check_vma=False,
    )
```

```python
import functools

import jax
import jax.numpy as jnp
import numpy as np
from jax import lax
from jax.experimental import pallas as pl
from jax.experimental.pallas import tpu as pltpu
from jax.sharding import PartitionSpec as P

BOTH = ("grp", "hlp")
F32 = jnp.float32
BF16 = jnp.bfloat16


def round_up(value, multiple):
    return -(-value // multiple) * multiple


class Plan:
    def __init__(self, groups, helpers):
        self.groups, self.helpers = groups, helpers
        self.half = helpers // 2
        self.ring = list(range(0, helpers, 2)) + list(range(helpers - 1, 0, -2))
        self.place = {h: i for i, h in enumerate(self.ring)}

    def at(self, helper, shift):
        return self.ring[(self.place[helper] + shift) % self.helpers]

    def sign(self, group):
        return 1 if group % 2 == 0 else -1

    def shift_perm(self, direction):
        return [
            (g * self.helpers + h, g * self.helpers + self.at(h, direction))
            for g in range(self.groups)
            for h in range(self.helpers)
        ]

    def side_perm(self):
        return [
            (g * self.helpers + h, g * self.helpers + self.at(h, self.sign(g)))
            for g in range(self.groups)
            for h in range(self.helpers)
        ]

    def partners(self):
        return np.array(
            [
                [[self.at(h, -self.sign(g) * d) for d in range(self.half + 1)] for h in range(self.helpers)]
                for g in range(2)
            ],
            np.int32,
        )

    def pieces(self):
        source = np.zeros((self.groups, self.helpers, self.helpers), np.int32)
        rows = np.zeros_like(source)
        for g in range(self.groups):
            for c in range(self.helpers):
                for e in range(self.helpers):
                    if e <= self.half:
                        source[g, c, e] = rows[g, c, e] = self.at(c, self.sign(g) * e)
                    else:
                        source[g, c, e] = c
                        rows[g, c, e] = self.at(c, -self.sign(g) * (e - self.half))
        return source, rows


def nt(a, b):
    return lax.dot_general(a, b, (((1,), (1,)), ((), ())), preferred_element_type=F32)


def nn(a, b):
    return jnp.dot(a, b, preferred_element_type=F32)


def build_kernel(
    firstcode_ref, secondcode_ref, schur_ref, lower_ref, factor_ref, contrib_ref, update_ref,
    out_ref, pairs, *, half, block, per_step, top, low, rows_per, rhs_half,
):
    step = pl.program_id(0)

    @pl.when(step == 0)
    def _():
        far = contrib_ref[...] - nt(lower_ref[...], factor_ref[...])
        for p in range(half):
            pairs[0, p] = schur_ref[p]
            pairs[1, p] = far.astype(BF16) if p == 0 else schur_ref[p].astype(F32).T.astype(BF16)

    def picker(code, rows):
        at = lax.broadcasted_iota(jnp.int32, (per_step * rows, block), 0) + step * (per_step * rows)
        return (code == at).astype(BF16)

    under = rows_per - low
    first = picker(firstcode_ref[...], top)

    def merge(upper, lower):
        n = upper.shape[1]
        upper = upper.reshape(per_step, top, n)
        lower = lower.reshape(per_step, under, n)
        middle = upper[:, low:] + lower[:, : top - low]
        rows = [upper[:, :low], middle, lower[:, top - low :]]
        rows = [r for r in rows if r.shape[1] > 0]
        return jnp.concatenate(rows, axis=1).reshape(per_step * rows_per, n).astype(BF16)

    for p in range(half):
        second = picker(secondcode_ref[p], under)
        out_ref[:, p * block : (p + 1) * block] = merge(nn(first, pairs[0, p]), nn(second, pairs[1, p]))
        if p == 0:
            out_ref[:, half * block :] = merge(
                nn(first, update_ref[:, :rhs_half]), nn(second, update_ref[:, rhs_half:])
            )


def assemble_kernel(
    source_ref, start_ref, recv_ref, rowidx_ref, rhsidx_ref, tilecol_ref, parent_ref, prhs_ref,
    out_ref, rhs_ref, wide, mixed, turned, outt,
    *, groups, helpers, devices, rows_per, block, owned, pitch, rhs_half,
):
    g = pl.program_id(0)
    half = helpers // 2
    lanes = half * block

    @pl.when(g == 0)
    def _():
        rhs_ref[...] = prhs_ref[...]
        turned[:, block:, :] = jnp.zeros((groups * helpers, pitch, owned), F32)

    wide[...] = recv_ref[...].astype(F32)

    row_iota = lax.broadcasted_iota(jnp.int32, (owned, helpers * rows_per), 0)
    for f in range(2):
        pick = (rhsidx_ref[f] == row_iota).astype(BF16)
        at = slice(f * rhs_half, (f + 1) * rhs_half)
        rhs_ref[:, at] += nn(pick, recv_ref[:, lanes:])

    def place(c, carry):
        for e in range(helpers):
            h = source_ref[(g * helpers + c) * helpers + e]
            first = pl.multiple_of(h * rows_per, 8)
            p = e % half
            mixed[e * rows_per : (e + 1) * rows_per, :] = wide[
                pl.ds(first, rows_per), p * block : (p + 1) * block
            ]
        pick = (rowidx_ref[0, c] == row_iota).astype(BF16)
        turned[g * helpers + c, :block, :] = nn(pick, mixed[...].astype(BF16)).T
        return carry

    lax.fori_loop(0, helpers, place, 0, unroll=2)

    blocks = groups * helpers
    col_iota = lax.broadcasted_iota(jnp.int32, (owned, blocks * pitch), 0)

    @pl.when(g == groups - 1)
    def _():
        def tile(t, carry):
            stacked = jnp.concatenate(
                [
                    turned[q, pl.ds(pl.multiple_of(start_ref[q * devices + t] * 8, 8), pitch), :]
                    for q in range(blocks)
                ],
                axis=0,
            ).astype(BF16)
            pick = (tilecol_ref[t] == col_iota).astype(BF16)
            outt[pl.ds(pl.multiple_of(t * owned, 8), owned), :] = nn(pick, stacked)
            return carry

        lax.fori_loop(0, devices, tile, 0, unroll=2)

        def turn(b, carry):
            at = pl.ds(pl.multiple_of(b * 128, 128), 128)
            out_ref[:, at] = parent_ref[:, at] + outt[at, :].T
            return carry

        lax.fori_loop(0, devices * owned // 128, turn, 0, unroll=2)


def on_device(
    pivot_inverse, cross_block, contrib_block, pivot_sources, contrib_sources, ext_map, parent_front, parent_rhs
):
    helpers = lax.axis_size("hlp")
    groups = lax.axis_size("grp")
    devices = helpers * groups
    plan = Plan(groups, helpers)
    half = plan.half
    group, helper = lax.axis_index("grp"), lax.axis_index("hlp")
    me = group * helpers + helper
    inverse, coupling, contrib = pivot_inverse[0], cross_block[0], contrib_block[0]
    pivots = inverse.shape[0]
    block, width = contrib.shape
    nsrc = pivot_sources.shape[2]
    owned, parent_width = parent_front.shape
    cap = max(1, 2 * width // (helpers * devices))
    rows_per = round_up(2 * cap, 8)
    pitch = round_up(cap, 8) + 8
    rhs_half = nsrc // 2
    order = jnp.asarray(plan.partners())[group % 2, helper]

    entries = ext_map[0]
    place_of = jnp.sum((entries[None, :] < entries[:, None]).astype(jnp.int32), axis=1)
    sorter = place_of[None, :] == jnp.arange(block)[:, None]
    in_order = jnp.sum(jnp.where(sorter, entries[None, :], 0), axis=1)
    sorter = sorter.astype(BF16)
    coupling = nn(sorter, coupling).astype(BF16)
    sources = nn(sorter, contrib_sources[0])

    own = jnp.concatenate([inverse, pivot_sources[0]], axis=1)
    ahead, behind = plan.shift_perm(1), plan.shift_perm(-1)
    ring = jnp.asarray(np.array(plan.ring, np.int32))
    place = jnp.asarray(np.array([plan.place[h] for h in range(helpers)], np.int32))[helper]
    arrived = [(own, helper)]
    forth = back = own
    for s in range(1, half):
        forth = lax.ppermute(forth, BOTH, ahead)
        back = lax.ppermute(back, BOTH, behind)
        arrived.append((forth, ring[(place - s) % helpers]))
        arrived.append((back, ring[(place + s) % helpers]))
        if s == 1:
            told = jnp.stack([in_order, place_of])
            told, forth, back = lax.optimization_barrier((told, forth, back))
            heard = lax.all_to_all(jnp.broadcast_to(told, (devices, 2, block)), BOTH, 0, 0, tiled=True)
    cut = pivots // 2
    last = jnp.concatenate(
        [lax.ppermute(forth[:cut], BOTH, ahead), lax.ppermute(back[cut:], BOTH, behind)], axis=0
    )
    arrived.append((last, ring[(place + half) % helpers]))
    full = inverse.shape[1]
    lower = jnp.zeros((block, full), BF16)
    gathered = jnp.zeros((full, full + nsrc), BF16)
    for piece, owner_of in arrived:
        part = nt(coupling, piece[:, :full]).astype(BF16)
        lower = lax.dynamic_update_slice(lower, part, (0, owner_of * pivots))
        gathered = lax.dynamic_update_slice(gathered, piece, (owner_of * pivots, 0))

    side = plan.side_perm()
    factors = [lower]
    for d in range(half):
        factors.append(lax.ppermute(factors[-1], BOTH, side))

    solved_all = nn(gathered[:, :full], gathered[:, full:]).astype(BF16)
    solved = lax.dynamic_slice(solved_all, (helper * pivots, 0), (pivots, nsrc))
    update = (sources - nn(lower, solved_all)).astype(BF16)

    maps = heard[:, 0]
    owners = maps // owned
    local = maps - owners * owned
    edges = jnp.arange(devices) * owned
    starts = jnp.sum((maps[:, None, :] < edges[None, :, None]).astype(jnp.int32), axis=2)
    before = jnp.sum(
        jnp.where(owners[:, :, None] == jnp.arange(devices)[None, None, :], starts[:, None, :], 0), axis=2
    )
    rank = jnp.arange(block)[None, :] - before

    top, low = round_up(cap, 8), cap // 8 * 8
    mine_first = lax.dynamic_index_in_dim(owners * top + rank, me, 0, keepdims=True)
    in_second = owners * (rows_per - low) + rank + (cap - low)
    mine_second = jnp.stack(
        [lax.dynamic_index_in_dim(in_second, group * helpers + order[d], 0, keepdims=True) for d in range(half)]
    )
    exact = lax.Precision.HIGHEST
    ranked = jnp.dot(sorter.astype(F32), contrib, precision=exact)
    columns = []
    for d in range(half + 1):
        to = lax.dynamic_index_in_dim(heard[:, 1], group * helpers + order[d], 0, keepdims=False)
        sort_columns = (to[:, None] == jnp.arange(block)[None, :]).astype(F32)
        part = lax.dynamic_slice(ranked, (0, order[d] * block), (block, block))
        columns.append(jnp.dot(part, sort_columns, precision=exact))
    schur = jnp.stack([(columns[d] - nt(lower, factors[d])).astype(BF16) for d in range(half)])
    message = half * block + rhs_half
    steps = max(1, devices * rows_per // 448)
    whole2 = pl.BlockSpec((block, block), lambda i: (0, 0))
    send = pl.pallas_call(
        functools.partial(
            build_kernel,
            half=half, block=block, per_step=devices // steps, top=top, low=low, rows_per=rows_per,
            rhs_half=rhs_half,
        ),
        grid=(steps,),
        in_specs=[
            pl.BlockSpec((1, block), lambda i: (0, 0)),
            pl.BlockSpec((half, 1, block), lambda i: (0, 0, 0)),
            pl.BlockSpec((half, block, block), lambda i: (0, 0, 0)),
            pl.BlockSpec((block, full), lambda i: (0, 0)),
            pl.BlockSpec((block, full), lambda i: (0, 0)),
            whole2,
            pl.BlockSpec((block, nsrc), lambda i: (0, 0)),
        ],
        out_specs=pl.BlockSpec((devices * rows_per // steps, message), lambda i: (i, 0)),
        out_shape=jax.ShapeDtypeStruct((devices * rows_per, message), BF16),
        scratch_shapes=[pltpu.VMEM((2, half, block, block), BF16)],
        compiler_params=pltpu.CompilerParams(vmem_limit_bytes=40 * 1024 * 1024),
        name="build",
    )(mine_first, mine_second, schur, lower, factors[half], columns[half], update)
    recv = lax.all_to_all(send.reshape(devices, rows_per, message), BOTH, 0, 0, tiled=True)
    recv = recv.reshape(devices * rows_per, message)

    mine = owners == me
    ranks = jnp.arange(cap)[None, :, None]
    hit = mine[:, None, :] & (rank[:, None, :] == ranks)
    slot_row = jnp.sum(jnp.where(hit, local[:, None, :] + 1, 0), axis=2) - 1
    slot_row = slot_row.reshape(groups, helpers, cap)
    source, row_block = plan.pieces()
    nothing = -jnp.ones((groups, helpers, helpers, rows_per), jnp.int32)
    rowidx = nothing
    for e in range(helpers):
        f = 0 if e < half else 1
        rows_of = jnp.take_along_axis(slot_row, jnp.asarray(row_block[:, :, e])[:, :, None], axis=1)
        rowidx = rowidx.at[:, :, e, f * cap : (f + 1) * cap].set(rows_of)
    rowidx = rowidx.reshape(groups, helpers, 1, helpers * rows_per)
    rhsidx = jnp.stack(
        [nothing[:, 0].at[:, :, f * cap : (f + 1) * cap].set(slot_row) for f in range(2)], axis=1
    ).reshape(groups * 2, 1, helpers * rows_per)
    slot = owners * pitch + rank + before % 8
    every = jnp.arange(devices * pitch)[None, :, None]
    tilecol = jnp.sum(jnp.where(slot[:, None, :] == every, local[:, None, :] + 1, 0), axis=2) - 1
    tilecol = tilecol.reshape(devices, devices, pitch).transpose(1, 0, 2)
    tilecol = tilecol.reshape(devices, 1, devices * pitch)

    rows_in = helpers * rows_per
    kernel = functools.partial(
        assemble_kernel,
        groups=groups, helpers=helpers, devices=devices, rows_per=rows_per, block=block, owned=owned,
        pitch=pitch, rhs_half=rhs_half,
    )
    front_out, rhs_out = pl.pallas_call(
        kernel,
        grid_spec=pltpu.PrefetchScalarGridSpec(
            num_scalar_prefetch=2,
            grid=(groups,),
            in_specs=[
                pl.BlockSpec((rows_in, message), lambda g, s, t: (g, 0)),
                pl.BlockSpec((1, helpers, 1, rows_in), lambda g, s, t: (g, 0, 0, 0)),
                pl.BlockSpec((2, 1, rows_in), lambda g, s, t: (g, 0, 0)),
                pl.BlockSpec((devices, 1, devices * pitch), lambda g, s, t: (0, 0, 0)),
                pl.BlockSpec((owned, parent_width), lambda g, s, t: (0, 0)),
                pl.BlockSpec((owned, nsrc), lambda g, s, t: (0, 0)),
            ],
            out_specs=[
                pl.BlockSpec((owned, parent_width), lambda g, s, t: (0, 0)),
                pl.BlockSpec((owned, nsrc), lambda g, s, t: (0, 0)),
            ],
            scratch_shapes=[
                pltpu.VMEM((rows_in, message), F32),
                pltpu.VMEM((rows_in, block), F32),
                pltpu.VMEM((groups * helpers, block + pitch, owned), F32),
                pltpu.VMEM((parent_width, owned), F32),
            ],
        ),
        out_shape=[
            jax.ShapeDtypeStruct((owned, parent_width), F32),
            jax.ShapeDtypeStruct((owned, nsrc), F32),
        ],
        compiler_params=pltpu.CompilerParams(vmem_limit_bytes=60 * 1024 * 1024),
        name="assemble",
    )(
        jnp.asarray(source.reshape(-1)), (starts // 8).reshape(-1), recv, rowidx, rhsidx, tilecol, parent_front, parent_rhs
    )
    return solved[None], front_out, rhs_out


def solution(mesh):
    return jax.shard_map(
        on_device,
        mesh=mesh,
        in_specs=(
            P("grp", "hlp", None),
            P("grp", "hlp", None),
            P("grp", "hlp", None),
            P("grp", "hlp", None),
            P("grp", "hlp", None),
            P("grp", "hlp"),
            P(("grp", "hlp"), None),
            P(("grp", "hlp"), None),
        ),
        out_specs=(P("grp", "hlp", None), P(("grp", "hlp"), None), P(("grp", "hlp"), None)),
        check_vma=False,
    )
```

```python
import functools

import jax
import jax.numpy as jnp
import numpy as np
from jax import lax
from jax.experimental import pallas as pl
from jax.experimental.pallas import tpu as pltpu
from jax.sharding import PartitionSpec as P

BOTH = ("grp", "hlp")
F32 = jnp.float32
BF16 = jnp.bfloat16


def round_up(value, multiple):
    return -(-value // multiple) * multiple


class Plan:
    def __init__(self, groups, helpers):
        self.groups, self.helpers = groups, helpers
        self.half = helpers // 2
        self.ring = list(range(0, helpers, 2)) + list(range(helpers - 1, 0, -2))
        self.place = {h: i for i, h in enumerate(self.ring)}

    def at(self, helper, shift):
        return self.ring[(self.place[helper] + shift) % self.helpers]

    def sign(self, group):
        return 1 if group % 2 == 0 else -1

    def shift_perm(self, direction):
        return [
            (g * self.helpers + h, g * self.helpers + self.at(h, direction))
            for g in range(self.groups)
            for h in range(self.helpers)
        ]

    def side_perm(self):
        return [
            (g * self.helpers + h, g * self.helpers + self.at(h, self.sign(g)))
            for g in range(self.groups)
            for h in range(self.helpers)
        ]

    def partners(self):
        return np.array(
            [
                [[self.at(h, -self.sign(g) * d) for d in range(self.half + 1)] for h in range(self.helpers)]
                for g in range(2)
            ],
            np.int32,
        )

    def pieces(self):
        source = np.zeros((self.groups, self.helpers, self.helpers), np.int32)
        rows = np.zeros_like(source)
        for g in range(self.groups):
            for c in range(self.helpers):
                for e in range(self.helpers):
                    if e <= self.half:
                        source[g, c, e] = rows[g, c, e] = self.at(c, self.sign(g) * e)
                    else:
                        source[g, c, e] = c
                        rows[g, c, e] = self.at(c, -self.sign(g) * (e - self.half))
        return source, rows


def nt(a, b):
    return lax.dot_general(a, b, (((1,), (1,)), ((), ())), preferred_element_type=F32)


def nn(a, b):
    return jnp.dot(a, b, preferred_element_type=F32)


def build_kernel(
    firstcode_ref, secondcode_ref, schur_ref, lower_ref, factor_ref, contrib_ref, update_ref,
    out_ref, pairs, *, half, block, per_step, top, low, rows_per, rhs_half,
):
    step = pl.program_id(0)

    @pl.when(step == 0)
    def _():
        far = contrib_ref[...] - nt(lower_ref[...], factor_ref[...])
        for p in range(half):
            pairs[0, p] = schur_ref[p]
            pairs[1, p] = far.astype(BF16) if p == 0 else schur_ref[p].astype(F32).T.astype(BF16)

    def picker(code, rows):
        at = lax.broadcasted_iota(jnp.int32, (per_step * rows, block), 0) + step * (per_step * rows)
        return (code == at).astype(BF16)

    under = rows_per - low
    first = picker(firstcode_ref[...], top)

    def merge(upper, lower):
        n = upper.shape[1]
        upper = upper.reshape(per_step, top, n)
        lower = lower.reshape(per_step, under, n)
        middle = upper[:, low:] + lower[:, : top - low]
        rows = [upper[:, :low], middle, lower[:, top - low :]]
        rows = [r for r in rows if r.shape[1] > 0]
        return jnp.concatenate(rows, axis=1).reshape(per_step * rows_per, n).astype(BF16)

    for p in range(half):
        second = picker(secondcode_ref[p], under)
        out_ref[:, p * block : (p + 1) * block] = merge(nn(first, pairs[0, p]), nn(second, pairs[1, p]))
        if p == 0:
            out_ref[:, half * block :] = merge(
                nn(first, update_ref[:, :rhs_half]), nn(second, update_ref[:, rhs_half:])
            )


def assemble_kernel(
    source_ref, start_ref, recv_ref, rowidx_ref, rhsidx_ref, tilecol_ref, parent_ref, prhs_ref,
    out_ref, rhs_ref, wide, mixed, turned, outt,
    *, groups, helpers, devices, rows_per, block, owned, pitch, rhs_half,
):
    g = pl.program_id(0)
    half = helpers // 2
    lanes = half * block

    @pl.when(g == 0)
    def _():
        rhs_ref[...] = prhs_ref[...]
        turned[:, block:, :] = jnp.zeros((groups * helpers, pitch, owned), F32)

    wide[...] = recv_ref[...].astype(F32)

    row_iota = lax.broadcasted_iota(jnp.int32, (owned, helpers * rows_per), 0)
    for f in range(2):
        pick = (rhsidx_ref[f] == row_iota).astype(BF16)
        at = slice(f * rhs_half, (f + 1) * rhs_half)
        rhs_ref[:, at] += nn(pick, recv_ref[:, lanes:])

    def place(c, carry):
        for e in range(helpers):
            h = source_ref[(g * helpers + c) * helpers + e]
            first = pl.multiple_of(h * rows_per, 8)
            p = e % half
            mixed[e * rows_per : (e + 1) * rows_per, :] = wide[
                pl.ds(first, rows_per), p * block : (p + 1) * block
            ]
        pick = (rowidx_ref[0, c] == row_iota).astype(BF16)
        turned[g * helpers + c, :block, :] = nn(pick, mixed[...].astype(BF16)).T
        return carry

    lax.fori_loop(0, helpers, place, 0, unroll=2)

    blocks = groups * helpers
    col_iota = lax.broadcasted_iota(jnp.int32, (owned, blocks * pitch), 0)

    @pl.when(g == groups - 1)
    def _():
        def tile(t, carry):
            stacked = jnp.concatenate(
                [
                    turned[q, pl.ds(pl.multiple_of(start_ref[q * devices + t] * 8, 8), pitch), :]
                    for q in range(blocks)
                ],
                axis=0,
            ).astype(BF16)
            pick = (tilecol_ref[t] == col_iota).astype(BF16)
            outt[pl.ds(pl.multiple_of(t * owned, 8), owned), :] = nn(pick, stacked)
            return carry

        lax.fori_loop(0, devices, tile, 0, unroll=2)

        def turn(b, carry):
            at = pl.ds(pl.multiple_of(b * 128, 128), 128)
            out_ref[:, at] = parent_ref[:, at] + outt[at, :].T
            return carry

        lax.fori_loop(0, devices * owned // 128, turn, 0, unroll=2)


def on_device(
    pivot_inverse, cross_block, contrib_block, pivot_sources, contrib_sources, ext_map, parent_front, parent_rhs
):
    helpers = lax.axis_size("hlp")
    groups = lax.axis_size("grp")
    devices = helpers * groups
    plan = Plan(groups, helpers)
    half = plan.half
    group, helper = lax.axis_index("grp"), lax.axis_index("hlp")
    me = group * helpers + helper
    inverse, coupling, contrib = pivot_inverse[0], cross_block[0], contrib_block[0]
    pivots = inverse.shape[0]
    block, width = contrib.shape
    nsrc = pivot_sources.shape[2]
    owned, parent_width = parent_front.shape
    cap = max(1, 2 * width // (helpers * devices))
    rows_per = round_up(2 * cap, 8)
    pitch = round_up(cap, 8) + 8
    rhs_half = nsrc // 2
    order = jnp.asarray(plan.partners())[group % 2, helper]

    entries = ext_map[0]
    place_of = jnp.sum((entries[None, :] < entries[:, None]).astype(jnp.int32), axis=1)
    sorter = place_of[None, :] == jnp.arange(block)[:, None]
    in_order = jnp.sum(jnp.where(sorter, entries[None, :], 0), axis=1)
    told = jnp.stack([in_order, place_of])
    sorter = sorter.astype(BF16)
    coupling = nn(sorter, coupling).astype(BF16)
    sources = nn(sorter, contrib_sources[0])

    own = jnp.concatenate([inverse, pivot_sources[0]], axis=1)
    ahead, behind = plan.shift_perm(1), plan.shift_perm(-1)
    ring = jnp.asarray(np.array(plan.ring, np.int32))
    place = jnp.asarray(np.array([plan.place[h] for h in range(helpers)], np.int32))[helper]
    arrived = [(own, helper)]
    forth = back = own
    for s in range(1, half):
        forth = lax.ppermute(forth, BOTH, ahead)
        back = lax.ppermute(back, BOTH, behind)
        arrived.append((forth, ring[(place - s) % helpers]))
        arrived.append((back, ring[(place + s) % helpers]))
    cut = pivots // 2
    last = jnp.concatenate(
        [lax.ppermute(forth[:cut], BOTH, ahead), lax.ppermute(back[cut:], BOTH, behind)], axis=0
    )
    arrived.append((last, ring[(place + half) % helpers]))
    full = inverse.shape[1]
    lower = jnp.zeros((block, full), BF16)
    pivot_all = jnp.zeros((full, nsrc), BF16)
    parts = []
    for piece, owner_of in arrived:
        part = nt(coupling, piece[:, :full]).astype(BF16)
        parts.append(part)
        lower = lax.dynamic_update_slice(lower, part, (0, owner_of * pivots))
        pivot_all = lax.dynamic_update_slice(pivot_all, piece[:, full:], (owner_of * pivots, 0))
    side = plan.side_perm()
    factors = [lower]
    for d in range(half):
        factors.append(lax.ppermute(factors[-1], BOTH, side))
        if d == 0:
            told, contrib, pivot_all, factors[1] = lax.optimization_barrier((told, contrib, pivot_all, factors[1]))
            heard = lax.all_to_all(jnp.broadcast_to(told, (devices, 2, block)), BOTH, 0, 0, tiled=True)

    solved_all = nn(jnp.concatenate([piece[:, :full] for piece, _ in arrived], axis=0), pivot_all).astype(BF16)
    solved = solved_all[:pivots]
    update = (sources - nn(jnp.concatenate(parts, axis=1), solved_all)).astype(BF16)

    maps = heard[:, 0]
    owners = maps // owned
    local = maps - owners * owned
    edges = jnp.arange(devices) * owned
    starts = jnp.sum((maps[:, None, :] < edges[None, :, None]).astype(jnp.int32), axis=2)
    before = jnp.sum(
        jnp.where(owners[:, :, None] == jnp.arange(devices)[None, None, :], starts[:, None, :], 0), axis=2
    )
    rank = jnp.arange(block)[None, :] - before

    top, low = round_up(cap, 8), cap // 8 * 8
    mine_first = lax.dynamic_index_in_dim(owners * top + rank, me, 0, keepdims=True)
    in_second = owners * (rows_per - low) + rank + (cap - low)
    mine_second = jnp.stack(
        [lax.dynamic_index_in_dim(in_second, group * helpers + order[d], 0, keepdims=True) for d in range(half)]
    )
    def terms(x):
        coarse = x.astype(BF16)
        return coarse, (x - coarse.astype(F32)).astype(BF16)

    columns = []
    for d in range(half + 1):
        to = lax.dynamic_index_in_dim(heard[:, 1], group * helpers + order[d], 0, keepdims=False)
        sort_columns = (to[:, None] == jnp.arange(block)[None, :]).astype(BF16)
        coarse, fine = terms(lax.dynamic_slice(contrib, (0, order[d] * block), (block, block)))
        ranked = nn(jnp.concatenate([coarse, fine], axis=0), sort_columns).astype(BF16)
        columns.append(nn(jnp.concatenate([sorter, sorter], axis=1), ranked))
    schur = jnp.stack([(columns[d] - nt(lower, factors[d])).astype(BF16) for d in range(half)])
    message = half * block + rhs_half
    steps = max(1, devices * rows_per // 448)
    whole2 = pl.BlockSpec((block, block), lambda i: (0, 0))
    send = pl.pallas_call(
        functools.partial(
            build_kernel,
            half=half, block=block, per_step=devices // steps, top=top, low=low, rows_per=rows_per,
            rhs_half=rhs_half,
        ),
        grid=(steps,),
        in_specs=[
            pl.BlockSpec((1, block), lambda i: (0, 0)),
            pl.BlockSpec((half, 1, block), lambda i: (0, 0, 0)),
            pl.BlockSpec((half, block, block), lambda i: (0, 0, 0)),
            pl.BlockSpec((block, full), lambda i: (0, 0)),
            pl.BlockSpec((block, full), lambda i: (0, 0)),
            whole2,
            pl.BlockSpec((block, nsrc), lambda i: (0, 0)),
        ],
        out_specs=pl.BlockSpec((devices * rows_per // steps, message), lambda i: (i, 0)),
        out_shape=jax.ShapeDtypeStruct((devices * rows_per, message), BF16),
        scratch_shapes=[pltpu.VMEM((2, half, block, block), BF16)],
        compiler_params=pltpu.CompilerParams(vmem_limit_bytes=40 * 1024 * 1024),
        name="build",
    )(mine_first, mine_second, schur, lower, factors[half], columns[half], update)
    recv = lax.all_to_all(send.reshape(devices, rows_per, message), BOTH, 0, 0, tiled=True)
    recv = recv.reshape(devices * rows_per, message)

    mine = owners == me
    ranks = jnp.arange(cap)[None, :, None]
    hit = mine[:, None, :] & (rank[:, None, :] == ranks)
    slot_row = jnp.sum(jnp.where(hit, local[:, None, :] + 1, 0), axis=2) - 1
    slot_row = slot_row.reshape(groups, helpers, cap)
    source, row_block = plan.pieces()

    def in_half(rows_of, f):
        ends = [(0, 0)] * (rows_of.ndim - 1) + [(f * cap, rows_per - (f + 1) * cap)]
        return jnp.pad(rows_of, ends, constant_values=-1)

    chosen = jnp.sum(
        jnp.where(
            jnp.asarray(row_block)[..., None, None] == jnp.arange(helpers)[:, None],
            slot_row[:, None, None],
            0,
        ),
        axis=3,
    )
    rowidx = jnp.concatenate([in_half(chosen[:, :, :half], 0), in_half(chosen[:, :, half:], 1)], axis=2)
    rowidx = rowidx.reshape(groups, helpers, 1, helpers * rows_per)
    rhsidx = jnp.stack([in_half(slot_row, f) for f in range(2)], axis=1)
    rhsidx = rhsidx.reshape(groups * 2, 1, helpers * rows_per)
    slot = owners * pitch + rank + before % 8
    every = jnp.arange(devices * pitch)[None, :, None]
    tilecol = jnp.sum(jnp.where(slot[:, None, :] == every, local[:, None, :] + 1, 0), axis=2) - 1
    tilecol = tilecol.reshape(devices, devices, pitch).transpose(1, 0, 2)
    tilecol = tilecol.reshape(devices, 1, devices * pitch)

    rows_in = helpers * rows_per
    kernel = functools.partial(
        assemble_kernel,
        groups=groups, helpers=helpers, devices=devices, rows_per=rows_per, block=block, owned=owned,
        pitch=pitch, rhs_half=rhs_half,
    )
    front_out, rhs_out = pl.pallas_call(
        kernel,
        grid_spec=pltpu.PrefetchScalarGridSpec(
            num_scalar_prefetch=2,
            grid=(groups,),
            in_specs=[
                pl.BlockSpec((rows_in, message), lambda g, s, t: (g, 0)),
                pl.BlockSpec((1, helpers, 1, rows_in), lambda g, s, t: (g, 0, 0, 0)),
                pl.BlockSpec((2, 1, rows_in), lambda g, s, t: (g, 0, 0)),
                pl.BlockSpec((devices, 1, devices * pitch), lambda g, s, t: (0, 0, 0)),
                pl.BlockSpec((owned, parent_width), lambda g, s, t: (0, 0)),
                pl.BlockSpec((owned, nsrc), lambda g, s, t: (0, 0)),
            ],
            out_specs=[
                pl.BlockSpec((owned, parent_width), lambda g, s, t: (0, 0)),
                pl.BlockSpec((owned, nsrc), lambda g, s, t: (0, 0)),
            ],
            scratch_shapes=[
                pltpu.VMEM((rows_in, message), F32),
                pltpu.VMEM((rows_in, block), F32),
                pltpu.VMEM((groups * helpers, block + pitch, owned), F32),
                pltpu.VMEM((parent_width, owned), F32),
            ],
        ),
        out_shape=[
            jax.ShapeDtypeStruct((owned, parent_width), F32),
            jax.ShapeDtypeStruct((owned, nsrc), F32),
        ],
        compiler_params=pltpu.CompilerParams(vmem_limit_bytes=60 * 1024 * 1024),
        name="assemble",
    )(
        jnp.asarray(source.reshape(-1)), (starts // 8).reshape(-1), recv, rowidx, rhsidx, tilecol, parent_front, parent_rhs
    )
    return solved[None], front_out, rhs_out


def solution(mesh):
    return jax.shard_map(
        on_device,
        mesh=mesh,
        in_specs=(
            P("grp", "hlp", None),
            P("grp", "hlp", None),
            P("grp", "hlp", None),
            P("grp", "hlp", None),
            P("grp", "hlp", None),
            P("grp", "hlp"),
            P(("grp", "hlp"), None),
            P(("grp", "hlp"), None),
        ),
        out_specs=(P("grp", "hlp", None), P(("grp", "hlp"), None), P(("grp", "hlp"), None)),
        check_vma=False,
    )
```

```python
import functools

import jax
import jax.numpy as jnp
import numpy as np
from jax import lax
from jax.experimental import pallas as pl
from jax.experimental.pallas import tpu as pltpu
from jax.sharding import PartitionSpec as P

BOTH = ("grp", "hlp")
F32 = jnp.float32
BF16 = jnp.bfloat16


def round_up(value, multiple):
    return -(-value // multiple) * multiple


class Plan:
    def __init__(self, groups, helpers):
        self.groups, self.helpers = groups, helpers
        self.half = helpers // 2
        self.ring = list(range(0, helpers, 2)) + list(range(helpers - 1, 0, -2))
        self.place = {h: i for i, h in enumerate(self.ring)}

    def at(self, helper, shift):
        return self.ring[(self.place[helper] + shift) % self.helpers]

    def sign(self, group):
        return 1 if group % 2 == 0 else -1

    def shift_perm(self, direction):
        return [
            (g * self.helpers + h, g * self.helpers + self.at(h, direction))
            for g in range(self.groups)
            for h in range(self.helpers)
        ]

    def side_perm(self):
        return [
            (g * self.helpers + h, g * self.helpers + self.at(h, self.sign(g)))
            for g in range(self.groups)
            for h in range(self.helpers)
        ]

    def partners(self):
        return np.array(
            [
                [[self.at(h, -self.sign(g) * d) for d in range(self.half + 1)] for h in range(self.helpers)]
                for g in range(2)
            ],
            np.int32,
        )

    def pieces(self):
        source = np.zeros((self.groups, self.helpers, self.helpers), np.int32)
        rows = np.zeros_like(source)
        for g in range(self.groups):
            for c in range(self.helpers):
                for e in range(self.helpers):
                    if e <= self.half:
                        source[g, c, e] = rows[g, c, e] = self.at(c, self.sign(g) * e)
                    else:
                        source[g, c, e] = c
                        rows[g, c, e] = self.at(c, -self.sign(g) * (e - self.half))
        return source, rows


def nt(a, b):
    return lax.dot_general(a, b, (((1,), (1,)), ((), ())), preferred_element_type=F32)


def nn(a, b):
    return jnp.dot(a, b, preferred_element_type=F32)


def build_kernel(
    firstcode_ref, secondcode_ref, schur_ref, lower_ref, factor_ref, contrib_ref, update_ref,
    out_ref, pairs, *, half, block, per_step, top, low, rows_per, rhs_half,
):
    step = pl.program_id(0)

    @pl.when(step == 0)
    def _():
        far = contrib_ref[...] - nt(lower_ref[...], factor_ref[...])
        for p in range(half):
            pairs[0, p] = schur_ref[p]
            pairs[1, p] = far.astype(BF16) if p == 0 else schur_ref[p].astype(F32).T.astype(BF16)

    def picker(code, rows):
        at = lax.broadcasted_iota(jnp.int32, (per_step * rows, block), 0) + step * (per_step * rows)
        return (code == at).astype(BF16)

    under = rows_per - low
    first = picker(firstcode_ref[...], top)

    def merge(upper, lower):
        n = upper.shape[1]
        upper = upper.reshape(per_step, top, n)
        lower = lower.reshape(per_step, under, n)
        middle = upper[:, low:] + lower[:, : top - low]
        rows = [upper[:, :low], middle, lower[:, top - low :]]
        rows = [r for r in rows if r.shape[1] > 0]
        return jnp.concatenate(rows, axis=1).reshape(per_step * rows_per, n).astype(BF16)

    for p in range(half):
        second = picker(secondcode_ref[p], under)
        out_ref[:, p * block : (p + 1) * block] = merge(nn(first, pairs[0, p]), nn(second, pairs[1, p]))
        if p == 0:
            out_ref[:, half * block :] = merge(
                nn(first, update_ref[:, :rhs_half]), nn(second, update_ref[:, rhs_half:])
            )


def assemble_kernel(
    source_ref, start_ref, recv_ref, rowidx_ref, rhsidx_ref, tilecol_ref, parent_ref, prhs_ref,
    out_ref, rhs_ref, wide, mixed, turned, outt,
    *, groups, helpers, devices, rows_per, block, owned, pitch, rhs_half,
):
    g = pl.program_id(0)
    half = helpers // 2
    lanes = half * block

    @pl.when(g == 0)
    def _():
        rhs_ref[...] = prhs_ref[...]
        turned[:, block:, :] = jnp.zeros((groups * helpers, pitch, owned), F32)

    wide[...] = recv_ref[...].astype(F32)

    row_iota = lax.broadcasted_iota(jnp.int32, (owned, helpers * rows_per), 0)
    for f in range(2):
        pick = (rhsidx_ref[f] == row_iota).astype(BF16)
        at = slice(f * rhs_half, (f + 1) * rhs_half)
        rhs_ref[:, at] += nn(pick, recv_ref[:, lanes:])

    def place(c, carry):
        for e in range(helpers):
            h = source_ref[(g * helpers + c) * helpers + e]
            first = pl.multiple_of(h * rows_per, 8)
            p = e % half
            mixed[e * rows_per : (e + 1) * rows_per, :] = wide[
                pl.ds(first, rows_per), p * block : (p + 1) * block
            ]
        pick = (rowidx_ref[0, c] == row_iota).astype(BF16)
        turned[g * helpers + c, :block, :] = nn(pick, mixed[...].astype(BF16)).T
        return carry

    lax.fori_loop(0, helpers, place, 0, unroll=4)

    blocks = groups * helpers
    col_iota = lax.broadcasted_iota(jnp.int32, (owned, blocks * pitch), 0)

    @pl.when(g == groups - 1)
    def _():
        def tile(t, carry):
            stacked = jnp.concatenate(
                [
                    turned[q, pl.ds(pl.multiple_of(start_ref[q * devices + t] * 8, 8), pitch), :]
                    for q in range(blocks)
                ],
                axis=0,
            ).astype(BF16)
            pick = (tilecol_ref[t] == col_iota).astype(BF16)
            outt[pl.ds(pl.multiple_of(t * owned, 8), owned), :] = nn(pick, stacked)
            return carry

        lax.fori_loop(0, devices, tile, 0, unroll=4)

        def turn(b, carry):
            at = pl.ds(pl.multiple_of(b * 128, 128), 128)
            out_ref[:, at] = parent_ref[:, at] + outt[at, :].T
            return carry

        lax.fori_loop(0, devices * owned // 128, turn, 0, unroll=2)


def on_device(
    pivot_inverse, cross_block, contrib_block, pivot_sources, contrib_sources, ext_map, parent_front, parent_rhs
):
    helpers = lax.axis_size("hlp")
    groups = lax.axis_size("grp")
    devices = helpers * groups
    plan = Plan(groups, helpers)
    half = plan.half
    group, helper = lax.axis_index("grp"), lax.axis_index("hlp")
    me = group * helpers + helper
    inverse, coupling, contrib = pivot_inverse[0], cross_block[0], contrib_block[0]
    pivots = inverse.shape[0]
    block, width = contrib.shape
    nsrc = pivot_sources.shape[2]
    owned, parent_width = parent_front.shape
    cap = max(1, 2 * width // (helpers * devices))
    rows_per = round_up(2 * cap, 8)
    pitch = round_up(cap, 8) + 8
    rhs_half = nsrc // 2
    order = jnp.asarray(plan.partners())[group % 2, helper]

    entries = ext_map[0]
    place_of = jnp.sum((entries[None, :] < entries[:, None]).astype(jnp.int32), axis=1)
    sorter = place_of[None, :] == jnp.arange(block)[:, None]
    in_order = jnp.sum(jnp.where(sorter, entries[None, :], 0), axis=1)
    told = jnp.stack([in_order, place_of])
    sorter = sorter.astype(BF16)
    coupling = nn(sorter, coupling).astype(BF16)
    sources = nn(sorter, contrib_sources[0])

    own = jnp.concatenate([inverse, pivot_sources[0]], axis=1)
    ahead, behind = plan.shift_perm(1), plan.shift_perm(-1)
    ring = jnp.asarray(np.array(plan.ring, np.int32))
    place = jnp.asarray(np.array([plan.place[h] for h in range(helpers)], np.int32))[helper]
    arrived = [(own, helper)]
    forth = back = own
    for s in range(1, half):
        forth = lax.ppermute(forth, BOTH, ahead)
        back = lax.ppermute(back, BOTH, behind)
        arrived.append((forth, ring[(place - s) % helpers]))
        arrived.append((back, ring[(place + s) % helpers]))
    cut = pivots // 2
    last = jnp.concatenate(
        [lax.ppermute(forth[:cut], BOTH, ahead), lax.ppermute(back[cut:], BOTH, behind)], axis=0
    )
    arrived.append((last, ring[(place + half) % helpers]))
    full = inverse.shape[1]
    lower = jnp.zeros((block, full), BF16)
    pivot_all = jnp.zeros((full, nsrc), BF16)
    parts = []
    for piece, owner_of in arrived:
        part = nt(coupling, piece[:, :full]).astype(BF16)
        parts.append(part)
        lower = lax.dynamic_update_slice(lower, part, (0, owner_of * pivots))
        pivot_all = lax.dynamic_update_slice(pivot_all, piece[:, full:], (owner_of * pivots, 0))
    side = plan.side_perm()
    factors = [lower]
    for d in range(half):
        factors.append(lax.ppermute(factors[-1], BOTH, side))
        if d == 0:
            told, contrib, pivot_all, factors[1] = lax.optimization_barrier((told, contrib, pivot_all, factors[1]))
            heard = lax.all_to_all(jnp.broadcast_to(told, (devices, 2, block)), BOTH, 0, 0, tiled=True)

    solved_all = nn(jnp.concatenate([piece[:, :full] for piece, _ in arrived], axis=0), pivot_all).astype(BF16)
    solved = solved_all[:pivots]
    update = (sources - nn(jnp.concatenate(parts, axis=1), solved_all)).astype(BF16)

    maps = heard[:, 0]
    owners = maps // owned
    local = maps - owners * owned
    edges = jnp.arange(devices) * owned
    starts = jnp.sum((maps[:, None, :] < edges[None, :, None]).astype(jnp.int32), axis=2)
    before = jnp.sum(
        jnp.where(owners[:, :, None] == jnp.arange(devices)[None, None, :], starts[:, None, :], 0), axis=2
    )
    rank = jnp.arange(block)[None, :] - before

    top, low = round_up(cap, 8), cap // 8 * 8
    mine_first = lax.dynamic_index_in_dim(owners * top + rank, me, 0, keepdims=True)
    in_second = owners * (rows_per - low) + rank + (cap - low)
    mine_second = jnp.stack(
        [lax.dynamic_index_in_dim(in_second, group * helpers + order[d], 0, keepdims=True) for d in range(half)]
    )
    def terms(x):
        coarse = x.astype(BF16)
        return coarse, (x - coarse.astype(F32)).astype(BF16)

    columns = []
    for d in range(half + 1):
        to = lax.dynamic_index_in_dim(heard[:, 1], group * helpers + order[d], 0, keepdims=False)
        sort_columns = (to[:, None] == jnp.arange(block)[None, :]).astype(BF16)
        coarse, fine = terms(lax.dynamic_slice(contrib, (0, order[d] * block), (block, block)))
        ranked = nn(jnp.concatenate([coarse, fine], axis=0), sort_columns).astype(BF16)
        columns.append(nn(jnp.concatenate([sorter, sorter], axis=1), ranked))
    schur = jnp.stack([(columns[d] - nt(lower, factors[d])).astype(BF16) for d in range(half)])
    message = half * block + rhs_half
    steps = max(1, devices * rows_per // 448)
    whole2 = pl.BlockSpec((block, block), lambda i: (0, 0))
    send = pl.pallas_call(
        functools.partial(
            build_kernel,
            half=half, block=block, per_step=devices // steps, top=top, low=low, rows_per=rows_per,
            rhs_half=rhs_half,
        ),
        grid=(steps,),
        in_specs=[
            pl.BlockSpec((1, block), lambda i: (0, 0)),
            pl.BlockSpec((half, 1, block), lambda i: (0, 0, 0)),
            pl.BlockSpec((half, block, block), lambda i: (0, 0, 0)),
            pl.BlockSpec((block, full), lambda i: (0, 0)),
            pl.BlockSpec((block, full), lambda i: (0, 0)),
            whole2,
            pl.BlockSpec((block, nsrc), lambda i: (0, 0)),
        ],
        out_specs=pl.BlockSpec((devices * rows_per // steps, message), lambda i: (i, 0)),
        out_shape=jax.ShapeDtypeStruct((devices * rows_per, message), BF16),
        scratch_shapes=[pltpu.VMEM((2, half, block, block), BF16)],
        compiler_params=pltpu.CompilerParams(vmem_limit_bytes=40 * 1024 * 1024),
        name="build",
    )(mine_first, mine_second, schur, lower, factors[half], columns[half], update)
    recv = lax.all_to_all(send.reshape(devices, rows_per, message), BOTH, 0, 0, tiled=True)
    recv = recv.reshape(devices * rows_per, message)

    mine = owners == me
    ranks = jnp.arange(cap)[None, :, None]
    hit = mine[:, None, :] & (rank[:, None, :] == ranks)
    slot_row = jnp.sum(jnp.where(hit, local[:, None, :] + 1, 0), axis=2) - 1
    slot_row = slot_row.reshape(groups, helpers, cap)
    source, row_block = plan.pieces()

    def in_half(rows_of, f):
        ends = [(0, 0)] * (rows_of.ndim - 1) + [(f * cap, rows_per - (f + 1) * cap)]
        return jnp.pad(rows_of, ends, constant_values=-1)

    chosen = jnp.sum(
        jnp.where(
            jnp.asarray(row_block)[..., None, None] == jnp.arange(helpers)[:, None],
            slot_row[:, None, None],
            0,
        ),
        axis=3,
    )
    rowidx = jnp.concatenate([in_half(chosen[:, :, :half], 0), in_half(chosen[:, :, half:], 1)], axis=2)
    rowidx = rowidx.reshape(groups, helpers, 1, helpers * rows_per)
    rhsidx = jnp.stack([in_half(slot_row, f) for f in range(2)], axis=1)
    rhsidx = rhsidx.reshape(groups * 2, 1, helpers * rows_per)
    slot = owners * pitch + rank + before % 8
    every = jnp.arange(devices * pitch)[None, :, None]
    tilecol = jnp.sum(jnp.where(slot[:, None, :] == every, local[:, None, :] + 1, 0), axis=2) - 1
    tilecol = tilecol.reshape(devices, devices, pitch).transpose(1, 0, 2)
    tilecol = tilecol.reshape(devices, 1, devices * pitch)

    rows_in = helpers * rows_per
    kernel = functools.partial(
        assemble_kernel,
        groups=groups, helpers=helpers, devices=devices, rows_per=rows_per, block=block, owned=owned,
        pitch=pitch, rhs_half=rhs_half,
    )
    front_out, rhs_out = pl.pallas_call(
        kernel,
        grid_spec=pltpu.PrefetchScalarGridSpec(
            num_scalar_prefetch=2,
            grid=(groups,),
            in_specs=[
                pl.BlockSpec((rows_in, message), lambda g, s, t: (g, 0)),
                pl.BlockSpec((1, helpers, 1, rows_in), lambda g, s, t: (g, 0, 0, 0)),
                pl.BlockSpec((2, 1, rows_in), lambda g, s, t: (g, 0, 0)),
                pl.BlockSpec((devices, 1, devices * pitch), lambda g, s, t: (0, 0, 0)),
                pl.BlockSpec((owned, parent_width), lambda g, s, t: (0, 0)),
                pl.BlockSpec((owned, nsrc), lambda g, s, t: (0, 0)),
            ],
            out_specs=[
                pl.BlockSpec((owned, parent_width), lambda g, s, t: (0, 0)),
                pl.BlockSpec((owned, nsrc), lambda g, s, t: (0, 0)),
            ],
            scratch_shapes=[
                pltpu.VMEM((rows_in, message), F32),
                pltpu.VMEM((rows_in, block), F32),
                pltpu.VMEM((groups * helpers, block + pitch, owned), F32),
                pltpu.VMEM((parent_width, owned), F32),
            ],
        ),
        out_shape=[
            jax.ShapeDtypeStruct((owned, parent_width), F32),
            jax.ShapeDtypeStruct((owned, nsrc), F32),
        ],
        compiler_params=pltpu.CompilerParams(vmem_limit_bytes=60 * 1024 * 1024),
        name="assemble",
    )(
        jnp.asarray(source.reshape(-1)), (starts // 8).reshape(-1), recv, rowidx, rhsidx, tilecol, parent_front, parent_rhs
    )
    return solved[None], front_out, rhs_out


def solution(mesh):
    return jax.shard_map(
        on_device,
        mesh=mesh,
        in_specs=(
            P("grp", "hlp", None),
            P("grp", "hlp", None),
            P("grp", "hlp", None),
            P("grp", "hlp", None),
            P("grp", "hlp", None),
            P("grp", "hlp"),
            P(("grp", "hlp"), None),
            P(("grp", "hlp"), None),
        ),
        out_specs=(P("grp", "hlp", None), P(("grp", "hlp"), None), P(("grp", "hlp"), None)),
        check_vma=False,
    )
```
